256 devices in a mesh: gr: 16 (over z, core), gc: 16 (over x, y).
Axes of the slice: x: 4, y: 4, z: 8, core: 2. Of those that a mesh axis runs over, the one named last changes fastest.
Arguments:
- projectors: bfloat16 [2, 65536, 9216], P(None, ('gr', 'gc')), may hold values from -0.046875 to 0.046875
- wavefunctions: bfloat16 [2, 65536, 512], P(None, ('gr', 'gc')), may hold values from -6 to 6
- coupling: float32 [512, 18, 18], P('gc'), may hold values from -1.5 to 1.5
- atom_order: int32 [512], replicated, may hold values from 0 to 511, each once
Outputs:
- coupled: float32 [9216, 512], P('gc', 'gr')
The draws below stay inside these ranges and needn't reach their ends.
Inputs may be any that keep to these rules, and one draw needn't show every extreme that they name: `atom_order`: a permutation of the atoms.
All inputs are finite; a program needn't handle non-finite values.
Results may differ from the reference program's by a relative error of at most 0.0003.
Values sent between devices are 32-bit elements; how exact they have to be, the bound alone decides.
A program may use at most 128 MiB of HBM per device.

```python
import jax
import jax.numpy as jnp
from jax import lax

ATOMS = 512
NH = 18
BANDS = 512
NKB = 9216
NPW = 65536


def spiked(drawn, key, source, target, parts, factor):
    def block_of(position):
        return (jnp.arange(drawn.shape[position]) // (drawn.shape[position] // parts)).reshape((-1,) + (1,) * (drawn.ndim - 1 - position))

    first = jax.random.permutation(key, parts)[block_of(target)]
    second = (block_of(target) + parts // 2) % parts
    return jnp.where((block_of(source) == first) | (block_of(source) == second), factor * drawn, drawn)


def block_scale(own_key, extent, cuts, least, largest):
    level, own = 1.0, jax.random.fold_in(own_key, 6)
    for dim, blocks in cuts:
        heights = jnp.exp(jax.random.uniform(jax.random.fold_in(own, dim), (blocks,), jnp.float32, least / len(cuts), largest / len(cuts)))
        level = level * jnp.repeat(heights, extent[dim] // blocks).reshape([-1 if axis == dim else 1 for axis in range(len(extent))])
    return level


def scatter_about(own_key, shape, width, reach, split=(), dtype=jnp.bfloat16):
    drawn = jax.random.normal(own_key, shape, jnp.float32) * width
    if len(split) > 0:
        drawn = block_scale(own_key, shape, split, -0.22, 0.18) * drawn
    return jnp.clip(drawn, min=-reach, max=reach).astype(dtype)


def heavy_noise(key, extent, width, reach, split, heavy, dtype=jnp.bfloat16):
    drawn = width * jax.random.normal(key, extent, jnp.float32)
    if split:
        drawn = drawn * block_scale(key, extent, split, -0.22, 0.18)
    return jnp.clip(spiked(drawn, jax.random.fold_in(key, 3), *heavy), -reach, reach).astype(dtype)


def setup_inputs(seed: int = 0) -> dict:
    seeds = jax.random.split(jax.random.key(seed), 5)
    return {
        "projectors": heavy_noise(seeds[0], (2, NPW, NKB), (4 * NPW) ** -0.5, 0.046875, ((1, 256),), (1, 2, 256, 6.0)),
        "wavefunctions": scatter_about(seeds[1], (2, NPW, BANDS), 1.0, 6.0, ((1, 256),)),
        "coupling": scatter_about(seeds[2], (ATOMS, NH, NH), NH ** -0.5, 1.5, ((0, 16),), jnp.float32),
        "atom_order": jax.random.permutation(seeds[3], ATOMS).astype(jnp.int32),
    }


def reference(projectors, wavefunctions, coupling, atom_order):
    shaped = projectors.reshape(2, NPW, ATOMS, NH)
    waves = wavefunctions.reshape(2 * NPW, BANDS)
    blocks = atom_order.reshape(-1, 32)

    def one_block(picked_ids):
        columns = jnp.take(shaped, picked_ids, axis=2).reshape(2 * NPW, 32 * NH)
        term = lax.dot_general(columns, waves, (((0,), (0,)), ((), ())), preferred_element_type=jnp.float32)
        return 2.0 * term

    becp = lax.map(one_block, blocks).reshape(ATOMS, NH, BANDS)
    coupled = jnp.einsum("kij,kjb->kib", coupling.astype(jnp.float32), becp, precision=lax.Precision.HIGHEST)
    return coupled.reshape(NKB, BANDS)
```

```python
import functools

import jax
import jax.numpy as jnp
from jax import lax
from jax.experimental import pallas as pl
from jax.experimental.pallas import tpu as pltpu
from jax.sharding import PartitionSpec as P

ATOMS = 512
NH = 18
BANDS = 512
NKB = 9216
KLOC = 512
MC = 512


def fold4(v):
    lane = lax.broadcasted_iota(jnp.int32, v[0].shape, 1)
    low = lane < 64
    even = (lane // 32) % 2 == 0
    roll = pltpu.roll
    lo = [jnp.where(low, v[q], roll(v[q + 2], 64, 1)) for q in range(2)]
    hi = [jnp.where(low, roll(v[q], 64, 1), v[q + 2]) for q in range(2)]
    u = []
    for a, b in (lo, hi):
        u.append(jnp.where(even, a, roll(b, 32, 1)))
        u.append(jnp.where(even, roll(a, 96, 1), b))
    return u


def local_kernel(order_ref, a_ref, w_ref, out_ref, p_ref, u_ref, a_v, asem, osem):
    cp = pltpu.make_async_copy(a_ref, a_v, asem)
    cp.start()
    cp.wait()
    for h in range(2):
        @pl.loop(0, NKB // MC)
        def _(m):
            lhs = a_v[:, pl.ds(pl.multiple_of(m * MC, MC), MC)]
            r = lax.dot_general(lhs, w_ref[:, h * 256:(h + 1) * 256], (((0,), (0,)), ((), ())),
                                preferred_element_type=jnp.float32)
            rows = pl.ds(pl.multiple_of(m * MC, MC), MC)
            p_ref[0, rows, :] = r[:, :128]
            p_ref[1, rows, :] = r[:, 128:]

        @pl.loop(0, 16)
        def _(gc):
            @pl.loop(0, 2)
            def _(t):
                for s in range(8):
                    v = []
                    for q in range(4):
                        start = order_ref[gc * 32 + q * 8 + s] * NH
                        v.append(p_ref[t, pl.ds(start, 24), :])
                    u = fold4(v)
                    n = 24 if s < 7 else 18
                    for d in range(4):
                        u_ref[h * 8 + t * 4 + d, gc, s * 18:s * 18 + n, :] = u[d][:n]
        pltpu.make_async_copy(u_ref.at[pl.ds(h * 8, 8)], out_ref.at[pl.ds(h * 8, 8)], osem.at[h]).start()
    for h in range(2):
        pltpu.make_async_copy(u_ref.at[pl.ds(h * 8, 8)], out_ref.at[pl.ds(h * 8, 8)], osem.at[h]).wait()


def local_units(order, a, w):
    return pl.pallas_call(
        local_kernel,
        out_shape=jax.ShapeDtypeStruct((16, 16, 144, 128), jnp.float32),
        in_specs=[
            pl.BlockSpec(memory_space=pltpu.SMEM),
            pl.BlockSpec(memory_space=pl.ANY),
            pl.BlockSpec(memory_space=pltpu.VMEM),
        ],
        out_specs=pl.BlockSpec(memory_space=pl.ANY),
        scratch_shapes=[
            pltpu.VMEM((2, NKB + 8, 128), jnp.float32),
            pltpu.VMEM((16, 16, 144, 128), jnp.float32),
            pltpu.VMEM((KLOC, NKB), jnp.bfloat16),
            pltpu.SemaphoreType.DMA,
            pltpu.SemaphoreType.DMA((2,)),
        ],
        compiler_params=pltpu.CompilerParams(vmem_limit_bytes=60 * 2**20),
        cost_estimate=pl.CostEstimate(flops=2 * KLOC * NKB * BANDS, bytes_accessed=30 * 2**20, transcendentals=0),
    )(order, a, w)


def shards(projectors, wavefunctions, coupling, atom_order):
    a = projectors.reshape(KLOC, NKB)
    w = wavefunctions.reshape(KLOC, BANDS)
    units = local_units(atom_order, a, w)
    units = units.reshape(256, 144, 128)
    mine = lax.psum_scatter(units, ("gr", "gc"), scatter_dimension=0, tiled=True)
    mine = 2.0 * mine.reshape(8, NH, 4, 32).transpose(2, 0, 1, 3).reshape(32, NH, 32)
    coupled = jnp.einsum("kij,kjb->kib", coupling, mine, precision=lax.Precision.HIGHEST)
    return coupled.reshape(576, 32)


def solution(mesh):
    return jax.shard_map(
        shards,
        mesh=mesh,
        in_specs=(
            P(None, ("gr", "gc"), None),
            P(None, ("gr", "gc"), None),
            P("gc", None, None),
            P(),
        ),
        out_specs=P("gc", "gr"),
        check_vma=False,
    )
```

```python
import jax
import jax.numpy as jnp
from jax import lax
from jax.experimental import pallas as pl
from jax.experimental.pallas import tpu as pltpu
from jax.sharding import PartitionSpec as P

MESH = pl.DeviceIdType.MESH
NH = 18
BANDS = 512
NKB = 9216
KLOC = 512
MC = 1152
CHUNKS = NKB // MC
ROWS = ((0, 48), (48, 96), (96, 144))
SCHEDULE = (
    "m0", "bar", "g0", "ds0", "g1", "ds1", "m1.0", "dw02", "c1.0.L0", "c1.1.L0", "m1.1", "dw00", "c1.2.L0", "c1.3.L0",
    "a1.0.L", "a1.0.S", "a1.1.L", "a1.1.S", "m1.2", "dw01", "b1.0.L", "b1.0.S", "b1.1.L", "b1.1.S", "m1.3", "dw12",
    "c1.0.f1", "c1.0.S0", "c1.1.S0", "g2", "ds2", "c1.1.f1", "dw10", "c1.2.S0", "a1.2.L", "a1.2.S", "a1.3.L",
    "a1.3.S", "g3", "ds3", "c1.2.f1", "dw11", "a1.0.1", "b1.2.L", "b1.2.S", "b1.3.L", "b1.3.S", "cb0", "c1.3.S0",
    "cb1", "c1.3.f1", "dw22", "b1.0.1", "cb2", "a1.1.1", "cb3", "c1.0.n1", "dw20", "a1.4.S", "a1.5.S", "cb4", "cb5",
    "c1.0.f2", "dw21", "b1.1.1", "b1.4.S", "b1.5.S", "a1.2.1", "dw32", "c1.1.n1", "c1.1.f2", "b1.2.1", "dw30",
    "a1.6.S", "a1.3.1", "a1.7.S", "dw31", "b1.6.S", "c1.2.n1", "b1.3.1", "c1.2.f2", "b1.7.S", "a1.0.E", "a1.4.L",
    "c1.3.n1", "b1.0.E", "c1.3.f2", "b1.4.L", "a1.1.E", "a2.0.L", "a2.0.S", "a1.5.L", "c1.0.n2", "c1.0.f3", "b1.1.E",
    "b2.0.L", "b2.0.S", "a1.2.E", "b1.5.L", "c1.1.n2", "a1.6.L", "c1.1.f3", "b1.2.E", "a1.3.E", "a2.1.L", "a2.1.S",
    "a1.7.L", "c1.2.n2", "b1.3.E", "b2.1.L", "b2.1.S", "c1.2.f3", "b1.6.L", "a1.4.1", "b1.7.L", "c1.3.n2", "a1.5.1",
    "b2.0.1", "b1.4.1", "c1.3.f3", "a2.0.1", "a1.6.1", "b1.5.1", "a2.1.1", "c1.0.E", "c2.0.L", "c2.1.L", "a1.7.1",
    "b2.1.1", "b1.6.1", "a1.4.E", "c1.1.E", "c2.0.S", "c2.1.S", "b1.7.1", "a1.5.E", "a2.2.L", "a2.2.S", "b1.4.E",
    "b2.0.E", "b3.0.L0", "a2.0.E", "a3.0.L0", "c1.2.E", "a1.6.E", "b1.5.E", "b2.2.L", "b2.2.S", "a2.1.E", "a3.0.S0",
    "c2.0.1", "c1.3.E", "a3.0.f1", "c2.1.1", "b1.6.E", "b1.7.E", "b2.3.L", "b2.3.S", "a1.7.E", "a2.3.L", "a2.3.S",
    "a2.2.1", "b2.1.E", "b3.0.S0", "b3.0.f1", "b2.2.1", "c2.0.E", "c3.0.L", "c3.0.S", "c2.1.E", "b2.3.1", "a2.3.1",
    "b2.2.E", "b3.0.f2", "b3.0.n1", "a2.2.E", "a3.0.f2", "a3.0.n1", "c3.0.1", "b2.3.E", "a2.3.E", "b3.0.f3",
    "b3.0.n2", "c3.0.E", "a3.0.f3", "a3.0.n2", "b3.0.E", "a3.0.E",
)


def fold4(v):
    lane = lax.broadcasted_iota(jnp.int32, v[0].shape, 1)
    low = lane < 64
    even = (lane // 32) % 2 == 0
    roll = pltpu.roll
    lo = [jnp.where(low, v[q], roll(v[q + 2], 64, 1)) for q in range(2)]
    hi = [jnp.where(low, roll(v[q], 64, 1), v[q + 2]) for q in range(2)]
    u = []
    for a, b in (lo, hi):
        u.append(jnp.where(even, a, roll(b, 32, 1)))
        u.append(jnp.where(even, roll(a, 96, 1), b))
    return u


def kernel(order_hbm, a_hbm, w_hbm, c_hbm, o_ref,
           p_ref, u_ref, d_ref, a_v, w_v, c_v, g_ref, pk, rk, t_ref,
           ra1, rb1, rc1, ra2, rb2, rc2, ra3, rb3, rc3,
           order, asem, wsem, csem, osem, ds_s, ds_r,
           a1s, a1r, b1s, b1r, c1s, c1r, a2s, a2r, b2s, b2r, c2s, c2r,
           a3s, a3r, b3s, b3r, c3s, c3r, ks_s, ks_r):
    gr, gc = lax.axis_index("gr"), lax.axis_index("gc")
    z, core = gr // 2, gr % 2
    x, y = gc // 4, gc % 4
    sg = 1 - 2 * core
    par = z % 2
    zt = z // 2
    quarter = par * 2 + core

    def xdev(d):
        return (gr, ((x + d + 4) % 4) * 4 + y)

    def ydev(d):
        return (gr, x * 4 + (y + d + 4) % 4)

    def zdev(d):
        return (((z + d + 8) % 8) * 2 + core, gc)

    partner = (gr + sg, gc)
    zpair = z + 1 - 2 * par
    pairdev = (zpair * 2 + core, gc)
    diagdev = (zpair * 2 + 1 - core, gc)

    tiles = [(zt + 2) % 4, (zt + 1 + 2 * par) % 4, (zt + 3 - 2 * par) % 4, zt]

    def kof(d):
        rel = ((par + d + 8) // 2) % 4
        odd = rel % 2
        half = rel // 2
        pos = odd * (1 + (par + half) % 2) + (1 - odd) * (3 - 3 * half)
        return 2 * pos + (par + d + 8) % 2

    kme = 6 + par

    def acopy(m):
        cols = pl.ds(pl.multiple_of(m * MC, 128), MC)
        return pltpu.make_async_copy(a_hbm.at[:, cols], a_v.at[:, cols], asem.at[m])

    def wcopy(t):
        return pltpu.make_async_copy(w_hbm.at[:, pl.ds(t * 128, 128)], w_v.at[t], wsem.at[t])

    with jax.named_scope("start"):
        for t in range(4):
            wcopy(t).start()
        acopy(0).start()
        ocopy = pltpu.make_async_copy(order_hbm, order, osem)
        ccopy = pltpu.make_async_copy(c_hbm, c_v, csem)
        barrier = pltpu.get_barrier_semaphore()
        greet = [xdev(1), xdev(-1), ydev(1), ydev(-1), zdev(1), zdev(-1), partner, diagdev]
        for dev in greet:
            pl.semaphore_signal(barrier, inc=1, device_id=dev, device_id_type=MESH)
    with jax.named_scope("waitw"):
        for t in range(4):
            wcopy(t).wait()
        acopy(1).start()
        acopy(2).start()
        ocopy.start()

    def matmul(h, first, last, wait):
        w = jnp.concatenate([w_v[tiles[2 * h]], w_v[tiles[2 * h + 1]]], axis=1)

        @pl.loop(first, last)
        def _(m):
            if wait:
                acopy(m).wait()

                @pl.when(m + 3 < CHUNKS)
                def _():
                    acopy(m + 3).start()
            lhs = a_v[:, pl.ds(pl.multiple_of(m * MC, 128), MC)]
            r = lax.dot_general(lhs, w, (((0,), (0,)), ((), ())), preferred_element_type=jnp.float32)
            rows = pl.ds(pl.multiple_of(m * MC, 128), MC)
            p_ref[0, rows, :] = r[:, :128]
            p_ref[1, rows, :] = r[:, 128:]

    def gather(kk):
        @pl.loop(0, 16)
        def _(g):
            for q in range(4):
                way = 1 - 2 * (q % 2)
                rx = (way * (g // 4 - x) + 4) % 4
                ry = (way * (g % 4 - y) + 4) % 4
                for s in range(8):
                    start = order[g * 32 + q * 8 + s] * NH
                    n = 24 if s < 7 else 18
                    u_ref[2 * kk + q // 2, q % 2, rx, ry, s * 18:s * 18 + n, :] = (
                        p_ref[kk % 2, pl.ds(start, n), :])

    def remote(src, dst, ssem, rsem, dev):
        return pltpu.make_async_remote_copy(src_ref=src, dst_ref=dst, send_sem=ssem, recv_sem=rsem,
                                            device_id=dev, device_id_type=MESH)

    def dcopy(kk, c):
        r0, r1 = ROWS[c]
        ks = pl.ds(2 * kk, 2)
        return remote(u_ref.at[ks, 1 - core, :, :, r0:r1, :], d_ref.at[ks, :, :, r0:r1, :],
                      ds_s, ds_r.at[kk, c], partner)

    def dsend(kk):
        for c in (2, 0, 1):
            dcopy(kk, c).start()

    def ring4(own, add, slot, ssem, rsem, dev):
        def copy(j):
            return remote(own((2, 1, 3)[j]), slot(j), ssem, rsem(min(j, 1)), dev(-sg if j == 2 else sg))

        def far():
            add(2, [])
            copy(0).start()

        def back():
            add(3, [])
            copy(2).start()

        def second():
            copy(0).wait_recv()
            add(1, [slot(0)])
            copy(1).start()

        def end():
            remote(slot(pl.ds(1, 2)), slot(pl.ds(1, 2)), ssem, rsem(1), dev(sg)).wait_recv()
            add(0, [slot(1), slot(2)])

        return {"L": far, "S": back, "1": second, "E": end}

    def ring8(own, add, slot, ssem, rsem):
        far = {0: 4 * sg, 1: 3 * sg, 2: 2 * sg, 3: sg, 5: -3 * sg, 6: -2 * sg, 4: -sg}
        sem = {0: 0, 1: 1, 2: 2, 3: 3, 4: 3, 5: 4, 6: 5}

        def copy(j):
            return remote(own(far[j]), slot(j), ssem, rsem(sem[j]), zdev(sg if j < 4 else -sg))

        def start(j):
            def run():
                add(far[j], [])
                copy(j).start()
            return run

        def step(before, j):
            def run():
                copy(before).wait_recv()
                add(far[j], [slot(before)])
                copy(j).start()
            return run

        def end():
            remote(slot(pl.ds(3, 2)), slot(pl.ds(3, 2)), ssem, rsem(3), zdev(sg)).wait_recv()
            add(0 * sg, [slot(3), slot(4)])

        return {"L0": start(0), "S0": start(5), "f1": step(0, 1), "f2": step(1, 2), "f3": step(2, 3),
                "n1": step(5, 6), "n2": step(6, 4), "E": end}

    def adder(own, more=None):
        def add(dest, extra):
            refs = ([more(dest)] if more is not None else []) + extra
            if refs:
                ref = own(dest)
                total = ref[...]
                for other in refs:
                    total = total + other[...]
                ref[...] = total
        return add

    def rows(c):
        return slice(*ROWS[c])

    def a1(k):
        own = lambda r: u_ref.at[k, core, r, :, rows(0), :]
        more = lambda r: d_ref.at[k, r, :, rows(0), :]
        return ring4(own, adder(own, more), lambda j: ra1.at[j, k],
                     a1s, lambda j: a1r.at[j, k], xdev)

    def b1(k):
        own = lambda r: u_ref.at[k, core, :, r, rows(1), :]
        more = lambda r: d_ref.at[k, :, r, rows(1), :]
        return ring4(own, adder(own, more), lambda j: rb1.at[j, k],
                     b1s, lambda j: b1r.at[j, k], ydev)

    def c1(i):
        r = (2, 3, 1, 0)[i]
        own = lambda d: u_ref.at[kof(d), core, r, :, rows(2), :]
        more = lambda d: d_ref.at[kof(d), r, :, rows(2), :]
        return ring8(own, adder(own, more), lambda j: rc1.at[j, r],
                     c1s, lambda j: c1r.at[j, r])

    def a2(i):
        ks = pl.ds(2 * i, 2)
        own = lambda r: u_ref.at[ks, core, 0, r, rows(0), :]
        return ring4(own, adder(own), lambda j: ra2.at[j, ks],
                     a2s, lambda j: a2r.at[j, i], ydev)

    def b2(i):
        ks = pl.ds(2 * i, 2)
        own = lambda r: u_ref.at[ks, core, r, 0, rows(1), :]
        return ring4(own, adder(own), lambda j: rb2.at[j, ks],
                     b2s, lambda j: b2r.at[j, i], xdev)

    def c2(i):
        ys = pl.ds(2 - 2 * i, 2)
        own = lambda r: u_ref.at[kme, core, r, ys, rows(2), :]
        return ring4(own, adder(own), lambda j: rc2.at[j, ys],
                     c2s, lambda j: c2r.at[j, i], xdev)

    def c3():
        own = lambda r: u_ref.at[kme, core, 0, r, rows(2), :]
        return ring4(own, adder(own), lambda j: rc3.at[j],
                     c3s, lambda j: c3r.at[j], ydev)

    def a3():
        own = lambda d: u_ref.at[kof(d), core, 0, 0, rows(0), :]
        return ring8(own, adder(own), lambda j: ra3.at[j], a3s, lambda j: a3r.at[j])

    def b3():
        own = lambda d: u_ref.at[kof(d), core, 0, 0, rows(1), :]
        return ring8(own, adder(own), lambda j: rb3.at[j], b3s, lambda j: b3r.at[j])

    def spread(i):
        if i == 0:
            ccopy.wait()
        for j in range(3 * i, 3 * i + 3):
            v = 2.0 * c_v[:, j, :]
            v = pltpu.roll(jnp.concatenate([v, v, v, v], axis=1), 128 - 8 * quarter, 1)
            for s in range(8):
                r = (s * NH + j) * 24
                p_ref[0, r:r + NH, :] = jnp.broadcast_to(v[:, s:s + 1], (NH, 128))

    todo = {}
    for k in range(4):
        todo[f"g{k}"] = lambda k=k: gather(k)
        todo[f"ds{k}"] = lambda k=k: dsend(k)
        for c in range(3):
            todo[f"dw{k}{c}"] = lambda k=k, c=c: dcopy(k, c).wait_recv()
        todo[f"m1.{k}"] = lambda k=k: matmul(1, 2 * k, 2 * k + 2, False)
    for name, rings in (("a1", [a1(k) for k in range(8)]), ("b1", [b1(k) for k in range(8)]), ("c1", [c1(i) for i in range(4)]),
                        ("a2", [a2(i) for i in range(4)]), ("b2", [b2(i) for i in range(4)]), ("c2", [c2(i) for i in range(2)]),
                        ("a3", [a3()]), ("b3", [b3()]), ("c3", [c3()])):
        for i, ring in enumerate(rings):
            for step, run in ring.items():
                todo[f"{name}.{i}.{step}"] = run
    todo["m0"] = lambda: matmul(0, 0, CHUNKS, True)
    def bar():
        ocopy.wait()
        ccopy.start()
        pl.semaphore_wait(barrier, len(greet))

    todo["bar"] = bar
    for i in range(6):
        todo[f"cb{i}"] = lambda i=i: spread(i)
    for name in SCHEDULE:
        with jax.named_scope(name):
            todo.pop(name)()
    assert not todo, list(todo)

    with jax.named_scope("couple"):
        for s in range(8):
            acc = None
            for j in range(NH):
                r = s * NH + j
                term = p_ref[0, r * 24:r * 24 + NH, :] * u_ref[kme, core, 0, 0, r:r + 1, :]
                acc = term if acc is None else acc + term
            g_ref[s * NH:s * NH + NH, :] = acc
    with jax.named_scope("pack"):
        for i in range(5):
            v = [g_ref[8 * t:8 * t + 8, :] for t in ((4 * i, 4 * i + 1, 4 * i + 2, 4 * i + 3) if i < 4 else (16, 17, 16, 17))]
            for d, u in enumerate(fold4(v)):
                pk[d, 8 * i:8 * i + 8, :] = u

    def kcopy(rel):
        dev = (partner, pairdev, diagdev)[rel]
        d = (par * 2 + 1 - core, (1 - par) * 2 + core, 3 - quarter)[rel]
        return remote(pk.at[d], rk.at[rel], ks_s, ks_r.at[rel], dev)

    for rel in (2, 1, 0):
        kcopy(rel).start()

    def unpack(ref, q):
        for t in range(18):
            tile = ref[8 * (t // 4):8 * (t // 4) + 8, :]
            if t % 4:
                tile = pltpu.roll(tile, 128 - 32 * (t % 4), 1)
            t_ref[pl.ds(pl.multiple_of(q * 144 + t * 8, 8), 8), :] = tile

    with jax.named_scope("unpack0"):
        unpack(pk.at[quarter], quarter)
    for rel, q in ((0, par * 2 + 1 - core), (1, (1 - par) * 2 + core), (2, 3 - quarter)):
        with jax.named_scope(f"k{rel}"):
            kcopy(rel).wait_recv()
        unpack(rk.at[rel], q)
    with jax.named_scope("turn"):
        o_ref[...] = jnp.transpose(t_ref[...])[:32, :]
    with jax.named_scope("drain"):
        for whole, sem in ((d_ref, ds_s), (ra1, a1s), (rb1, b1s), (rc1, c1s), (ra2, a2s), (rb2, b2s), (rc2, c2s),
                           (ra3, a3s), (rb3, b3s), (rc3, c3s), (rk, ks_s)):
            remote(whole, whole, sem, ks_r.at[0], partner).wait_send()


def shards(projectors, wavefunctions, coupling, atom_order):
    a = projectors.reshape(KLOC, NKB)
    w = wavefunctions.reshape(KLOC, BANDS)
    f32 = jnp.float32
    dma = pltpu.SemaphoreType.DMA
    any_spec = pl.BlockSpec(memory_space=pltpu.HBM)
    sems = []
    for shape in ((2, 8), (2, 8), (6, 4), (2, 4), (2, 4), (2, 2), (6,), (6,), (2,), (3,)):
        sems += [dma, dma(shape)]
    out = pl.pallas_call(
        kernel,
        out_shape=pltpu.VMEM((32, 576), f32),
        in_specs=[any_spec, any_spec, any_spec, any_spec],
        out_specs=pl.BlockSpec(memory_space=pltpu.VMEM),
        scratch_shapes=[
            pltpu.VMEM((2, NKB + 8, 128), f32),
            pltpu.VMEM((8, 2, 4, 4, 144, 128), f32),
            pltpu.VMEM((8, 4, 4, 144, 128), f32),
            pltpu.VMEM((KLOC, NKB), jnp.bfloat16),
            pltpu.VMEM((4, KLOC, 128), jnp.bfloat16),
            pltpu.VMEM((NH, NH, 32), f32),
            pltpu.VMEM((144, 128), f32),
            pltpu.VMEM((4, 40, 128), f32),
            pltpu.VMEM((3, 40, 128), f32),
            pltpu.VMEM((576, 128), f32),
            pltpu.VMEM((3, 8, 4, 48, 128), f32),
            pltpu.VMEM((3, 8, 4, 48, 128), f32),
            pltpu.VMEM((7, 4, 4, 48, 128), f32),
            pltpu.VMEM((3, 8, 48, 128), f32),
            pltpu.VMEM((3, 8, 48, 128), f32),
            pltpu.VMEM((3, 4, 48, 128), f32),
            pltpu.VMEM((7, 48, 128), f32),
            pltpu.VMEM((7, 48, 128), f32),
            pltpu.VMEM((3, 48, 128), f32),
            pltpu.SMEM((512,), jnp.int32),
            dma((CHUNKS,)),
            dma((4,)),
            dma,
            dma,
            dma,
            dma((4, 3)),
        ] + sems,
        compiler_params=pltpu.CompilerParams(
            vmem_limit_bytes=62500000, collective_id=0, has_side_effects=True),
        cost_estimate=pl.CostEstimate(flops=2 * KLOC * NKB * BANDS, bytes_accessed=10 * 2**20, transcendentals=0),
    )(atom_order, a, w, coupling.transpose(1, 2, 0))
    return out.T


def solution(mesh):
    return jax.shard_map(
        shards,
        mesh=mesh,
        in_specs=(
            P(None, ("gr", "gc"), None),
            P(None, ("gr", "gc"), None),
            P("gc", None, None),
            P(),
        ),
        out_specs=P("gc", "gr"),
        check_vma=False,
    )
```

```python
import functools

import jax
import jax.numpy as jnp
from jax import lax
from jax.experimental import pallas as pl
from jax.experimental.pallas import tpu as pltpu
from jax.sharding import PartitionSpec as P

MESH = pl.DeviceIdType.MESH
NH = 18
BANDS = 512
NKB = 9216
KLOC = 512
MC = 1152
CHUNKS = NKB // MC
ROWS = (slice(0, 48), slice(48, 96), slice(96, 144))


def fold4(v):
    lane = lax.broadcasted_iota(jnp.int32, v[0].shape, 1)
    low = lane < 64
    even = (lane // 32) % 2 == 0
    roll = pltpu.roll
    lo = [jnp.where(low, v[q], roll(v[q + 2], 64, 1)) for q in range(2)]
    hi = [jnp.where(low, roll(v[q], 64, 1), v[q + 2]) for q in range(2)]
    u = []
    for a, b in (lo, hi):
        u.append(jnp.where(even, a, roll(b, 32, 1)))
        u.append(jnp.where(even, roll(a, 96, 1), b))
    return u


def kernel(order_hbm, a_hbm, w_hbm, c_hbm, o_ref,
           p_ref, u_ref, d_ref, a_v, w_v, c_v, g_ref, pk, rk, t_ref,
           ra1, rb1, rc1, ra2, rb2, rc2, ra3, rb3, rc3,
           order, asem, wsem, csem, osem, ds_s, ds_r,
           a1s, a1r, b1s, b1r, c1s, c1r, a2s, a2r, b2s, b2r, c2s, c2r,
           a3s, a3r, b3s, b3r, c3s, c3r, ks_s, ks_r):
    gr, gc = lax.axis_index("gr"), lax.axis_index("gc")
    z, core = gr // 2, gr % 2
    x, y = gc // 4, gc % 4
    half = (core + x + y + z) % 2
    sg = 1 - 2 * half
    par = z % 2
    zt = z // 2
    quarter = par * 2 + half

    def xdev(d):
        return (z * 2 + (core + d + 4) % 2, ((x + d + 4) % 4) * 4 + y)

    def ydev(d):
        return (z * 2 + (core + d + 4) % 2, x * 4 + (y + d + 4) % 4)

    def pdev(d):
        return (z * 2 + (core + d + 4) % 2, (1 - half) * xdev(d)[1] + half * ydev(d)[1])

    def qdev(d):
        return (z * 2 + (core + d + 4) % 2, half * xdev(d)[1] + (1 - half) * ydev(d)[1])

    def zdev(d):
        return (((z + d + 8) % 8) * 2 + (core + d + 8) % 2, gc)

    partner = (z * 2 + 1 - core, gc)
    zpair = z + 1 - 2 * par
    pairdev = (zpair * 2 + 1 - core, gc)
    diagdev = (zpair * 2 + core, gc)

    tiles = [(zt + 2) % 4, (zt + 1 + 2 * par) % 4, (zt + 3 - 2 * par) % 4, zt]

    def kof(d):
        rel = ((par + d + 8) // 2) % 4
        odd = rel % 2
        up = rel // 2
        pos = odd * (1 + (par + up) % 2) + (1 - odd) * (3 - 3 * up)
        return 2 * pos + (par + d + 8) % 2

    kme = 6 + par

    def acopy(m):
        cols = pl.ds(pl.multiple_of(m * MC, 128), MC)
        return pltpu.make_async_copy(a_hbm.at[:, cols], a_v.at[:, cols], asem.at[m % 5])

    def wcopy(t):
        cols = pl.ds(pl.multiple_of(tiles[t] * 128, 128), 128)
        return pltpu.make_async_copy(w_hbm.at[:, cols], w_v.at[t], wsem.at[t])

    for t in range(2):
        wcopy(t).start()
    acopy(0).start()
    ocopy = pltpu.make_async_copy(order_hbm, order, osem)
    ccopy = pltpu.make_async_copy(c_hbm, c_v, csem)
    barrier = pltpu.get_barrier_semaphore()
    greet = [xdev(1), xdev(-1), xdev(2), ydev(1), ydev(-1), ydev(2), zdev(1), zdev(-1), zdev(2), zdev(-2), partner, diagdev]
    for dev in greet:
        pl.semaphore_signal(barrier, inc=1, device_id=dev, device_id_type=MESH)
    acopy(1).start()
    for t in range(2):
        wcopy(t).wait()
    for m in range(2, 4):
        acopy(m).start()
    for t in range(2, 4):
        wcopy(t).start()
    ocopy.start()

    def matmul(h, first, last, wait):
        w = jnp.concatenate([w_v[2 * h], w_v[2 * h + 1]], axis=1)

        @pl.loop(first, last)
        def _(m):
            if wait:
                acopy(m).wait()

                @pl.when(m + 4 < CHUNKS)
                def _():
                    acopy(m + 4).start()
            lhs = a_v[:, pl.ds(pl.multiple_of(m * MC, 128), MC)]
            r = lax.dot_general(lhs, w, (((0,), (0,)), ((), ())), preferred_element_type=jnp.float32)
            rows = pl.ds(pl.multiple_of(m * MC, 128), MC)
            p_ref[0, rows, :] = r[:, :128]
            p_ref[1, rows, :] = r[:, 128:]

    def gather(kk, zs):
        @pl.loop(0, 16)
        def _(g):
            for zl in zs:
                for h in range(2):
                    way = 1 - 2 * h
                    rx = (way * (g // 4 - x) + 4) % 4
                    ry = (way * (g % 4 - y) + 4) % 4
                    p, q = (rx, ry) if h == 0 else (ry, rx)
                    for s in range(8):
                        start = order[g * 32 + (2 * zl + h) * 8 + s] * NH
                        n = 24 if s < 7 else 18
                        u_ref[2 * kk + zl, h, p, q, s * 18:s * 18 + n, :] = p_ref[kk % 2, pl.ds(start, n), :]

    def remote(src, dst, ssem, rsem, dev):
        return pltpu.make_async_remote_copy(src_ref=src, dst_ref=dst, send_sem=ssem, recv_sem=rsem,
                                            device_id=dev, device_id_type=MESH)

    def dcopy(kk, c):
        ks = pl.ds(2 * kk, 2)
        return remote(u_ref.at[ks, 1 - half, :, :, ROWS[c], :], d_ref.at[ks, :, :, ROWS[c], :],
                      ds_s, ds_r.at[kk, c], partner)

    def dfirst(h, c):
        k = (par + h) % 2
        return remote(u_ref.at[k, 1 - half, :, :, ROWS[c], :], d_ref.at[k, :, :, ROWS[c], :],
                      ds_s, ds_r.at[4 * h, c], partner)

    def make(kk):
        gather(kk, (0, 1))
        for c in (0, 2, 1):
            dcopy(kk, c).start()

    def make_first(h):
        gather(0, ((par + h) % 2,))
        for c in (0, 2, 1):
            dfirst(h, c).start()

    def ring4(own, add, slot, ssem, rsem, dev, direct=False):
        def copy(j):
            if direct:
                return remote(own((2, 1, 3)[j]), slot(j), ssem, rsem(0), dev((2, sg, -sg)[j]))
            return remote(own((2, 1, 3)[j]), slot(j), ssem, rsem(min(j, 1)), dev(-sg if j == 2 else sg))

        def far():
            add(2, [])
            copy(0).start()

        def back():
            add(3, [])
            copy(2).start()

        def second():
            if not direct:
                copy(0).wait_recv()
                add(1, [slot(0)])
            copy(1).start()

        def end():
            first = 0 if direct else 1
            landed = slot(pl.ds(first, 3 - first))
            remote(landed, landed, ssem, rsem(first), dev(sg)).wait_recv()
            add(0, [slot(j) for j in range(first, 3)])

        return far, back, second, end

    def ring8(own, add, slot, ssem, rsem):
        far = {0: 4 * sg, 1: 3 * sg, 2: 2 * sg, 3: sg, 5: -3 * sg, 6: -2 * sg, 4: -sg}
        sem = {0: 0, 1: 1, 2: 2, 3: 3, 4: 3, 5: 4, 6: 5}

        def copy(j):
            return remote(own(far[j]), slot(j), ssem, rsem(sem[j]), zdev(sg if j < 4 else -sg))

        def start(j):
            def run():
                add(far[j], [])
                copy(j).start()
            return run

        def step(before, j):
            def run():
                copy(before).wait_recv()
                add(far[j], [slot(before)])
                copy(j).start()
            return run

        def end():
            remote(slot(pl.ds(3, 2)), slot(pl.ds(3, 2)), ssem, rsem(3), zdev(sg)).wait_recv()
            add(0 * sg, [slot(3), slot(4)])

        return start(0), start(5), step(0, 1), step(1, 2), step(2, 3), step(5, 6), step(6, 4), end

    def ring8_short(own, add, slot, ssem, rsem):
        far = (4 * sg, 3 * sg, -3 * sg, -2 * sg, 2 * sg, sg, -sg)
        dev = (2 * sg, sg, -2 * sg, -sg, 2 * sg, sg, -sg)
        group = (0, 0, 1, 1, 2, 2, 2)

        def copy(j):
            return remote(own(far[j]), slot(j), ssem, rsem(group[j]), zdev(dev[j]))

        def wait(first, n):
            landed = slot(pl.ds(first, n))
            remote(landed, landed, ssem, rsem(group[first]), zdev(sg)).wait_recv()
            return [slot(j) for j in range(first, first + n)]

        def join(first, j):
            def run():
                add(far[j], wait(first, 2))
                copy(j).start()
            return run

        def end():
            add(0 * sg, wait(4, 3))

        return (copy(0).start, copy(1).start, copy(2).start, copy(3).start, join(0, 4), copy(5).start, join(2, 6), end)

    def adder(own, more=None):
        def add(dest, extra):
            refs = ([more(dest)] if more is not None else []) + extra
            if refs:
                ref = own(dest)
                total = ref[...]
                for other in refs:
                    total = total + other[...]
                ref[...] = total
        return add

    def a1(k):
        at = (par + k) % 2 if k < 2 else k
        own = lambda r: u_ref.at[at, half, r, :, ROWS[0], :]
        more = lambda r: d_ref.at[at, r, :, ROWS[0], :]
        return ring4(own, adder(own, more), lambda j: ra1.at[j, k],
                     a1s, lambda j: a1r.at[j, k], pdev)

    def b1(k):
        at = (par + k) % 2 if k < 2 else k
        own = lambda r: u_ref.at[at, half, :, r, ROWS[1], :]
        more = lambda r: d_ref.at[at, :, r, ROWS[1], :]
        return ring4(own, adder(own, more), lambda j: rb1.at[j, k],
                     b1s, lambda j: b1r.at[j, k], qdev)

    def c1(i):
        r = (2, 3, 1, 0)[i]
        own = lambda d: u_ref.at[kof(d), half, r, :, ROWS[2], :]
        more = lambda d: d_ref.at[kof(d), r, :, ROWS[2], :]
        return ring8(own, adder(own, more), lambda j: rc1.at[j, r],
                     c1s, lambda j: c1r.at[j, r])

    def a2(i):
        ks = pl.ds(2 * i, 2)
        own = lambda r: u_ref.at[ks, half, 0, r, ROWS[0], :]
        return ring4(own, adder(own), lambda j: ra2.at[j, ks],
                     a2s, lambda j: a2r.at[j, i], qdev, direct=i in ())

    def b2(i):
        ks = pl.ds(2 * i, 2)
        own = lambda r: u_ref.at[ks, half, r, 0, ROWS[1], :]
        return ring4(own, adder(own), lambda j: rb2.at[j, ks],
                     b2s, lambda j: b2r.at[j, i], pdev, direct=i in ())

    def c2(i):
        ys = pl.ds(2 - 2 * i, 2)
        own = lambda r: u_ref.at[kme, half, r, ys, ROWS[2], :]
        return ring4(own, adder(own), lambda j: rc2.at[j, ys],
                     c2s, lambda j: c2r.at[j, i], pdev)

    def c3():
        own = lambda r: u_ref.at[kme, half, 0, r, ROWS[2], :]
        return ring4(own, adder(own), lambda j: rc3.at[j],
                     c3s, lambda j: c3r.at[j], qdev, direct=True)

    def a3():
        own = lambda d: u_ref.at[kof(d), half, 0, 0, ROWS[0], :]
        return ring8_short(own, adder(own), lambda j: ra3.at[j], a3s, lambda j: a3r.at[j])

    def b3():
        own = lambda d: u_ref.at[kof(d), half, 0, 0, ROWS[1], :]
        return ring8_short(own, adder(own), lambda j: rb3.at[j], b3s, lambda j: b3r.at[j])

    def spread(i):
        if i == 0:
            ccopy.wait()
        for j in range(3 * i, 3 * i + 3):
            v = 2.0 * c_v[:, j, :]
            v = pltpu.roll(jnp.concatenate([v, v, v, v], axis=1), 128 - 8 * quarter, 1)
            for s in range(8):
                r = (s * NH + j) * 24
                p_ref[0, r:r + NH, :] = jnp.broadcast_to(v[:, s:s + 1], (NH, 128))

    def bar():
        ocopy.wait()
        ccopy.start()
        for t in range(2, 4):
            wcopy(t).wait()
        pl.semaphore_wait(barrier, len(greet))

    def each(f, n):
        return [functools.partial(f, i) for i in range(n)]

    m0 = functools.partial(matmul, 0, 0, CHUNKS, True)
    m1 = [functools.partial(matmul, 1, 2 * i, 2 * i + 2, False) for i in range(4)]
    g0, g, cb = each(make_first, 2), each(make, 4), each(spread, 6)
    w0 = [[functools.partial(lambda h, c: dfirst(h, c).wait_recv(), h, c) for c in range(3)] for h in range(2)]
    wd = [[functools.partial(lambda k, c: dcopy(k, c).wait_recv(), k, c) for c in range(3)] for k in range(4)]
    ra, rb, rc = [a1(k) for k in range(8)], [b1(k) for k in range(8)], [c1(i) for i in range(4)]
    sa, sb, sc = [a2(i) for i in range(4)], [b2(i) for i in range(4)], [c2(i) for i in range(2)]
    ta, tb, tc = a3(), b3(), c3()
    for run in (
        m0, bar, g0[0], g0[1], g[1], w0[0][0], ra[0][1], ra[0][0], m1[0], w0[0][1], rb[0][0], rb[0][1], w0[0][2],
        rc[2][0], m1[1], rc[0][0], w0[1][0], ra[1][0], ra[1][1], m1[2], rc[1][0], w0[1][2], rc[3][0], wd[1][0],
        ra[2][0], ra[3][1], w0[1][1], rb[1][0], ra[3][0], m1[3], ra[0][2], g[2], wd[1][1], rb[2][0], wd[1][2],
        rb[2][1], rc[2][1], rc[0][2], rb[3][0], rc[1][1], rc[2][2], rb[1][1], wd[2][0], rc[0][1], ra[2][1], g[3],
        rb[3][1], ra[4][1], ra[4][0], wd[2][2], wd[2][1], rc[1][2], ra[5][1], rb[1][2], rb[3][2], rc[2][5], ra[2][2],
        ra[0][3], wd[3][0], ra[1][2], wd[3][2], rb[4][0], rb[5][0], rb[4][1], rb[2][2], wd[3][1], cb[0], rc[0][3],
        rc[3][2], ra[5][0], rb[0][2], rb[6][0], rb[7][0], cb[1], ra[3][2], ra[7][0], rc[2][3], rc[1][5], ra[2][3],
        rc[0][5], ra[1][3], rb[7][1], rb[4][2], ra[4][2], ra[5][2], ra[6][0], sa[0][0], rc[1][3], rc[3][1], rb[1][3],
        rc[1][6], rb[5][2], rb[0][3], ra[3][3], rb[3][3], rb[5][1], rb[6][2], rb[6][1], rc[0][4], cb[4], sb[0][0],
        rb[2][3], sa[1][0], rc[3][3], rb[7][2], sa[0][1], rb[4][3], sb[1][0], ra[7][2], sa[0][2], ra[4][3], ra[7][1],
        rc[0][6], ra[5][3], ra[6][1], rc[3][5], ra[6][2], rb[5][3], sb[2][0], sb[0][1], rc[1][4], rc[2][6], rc[2][4],
        sb[0][2], rc[3][4], sa[1][1], sa[1][2], sa[2][0], rb[7][3], rc[0][7], sc[1][0], cb[3], sb[1][2], cb[2],
        sb[1][1], rb[6][3], sc[0][0], sb[2][1], rc[3][6], sb[3][0], ra[7][3], ra[6][3], sa[3][0], sa[0][3], sb[2][2],
        sa[1][3], sa[2][2], ta[0], sa[2][1], cb[5], sb[0][3], tb[0], sb[3][1], rc[1][7], sa[3][1], sb[1][3], ta[1],
        tb[1], rc[2][7], sc[0][1], sc[1][2], sc[0][2], tb[2], sc[1][1], sb[3][2], ta[2], sa[3][2], sb[2][3], tb[3],
        rc[3][7], sa[2][3], ta[3], ta[4], sc[0][3], tc[0], tb[4], tc[1], sa[3][3], ta[5], sb[3][3], sc[1][3], tb[5],
        tb[6], tc[2], ta[6], tc[3], tb[7], ta[7],
    ):
        run()

    for s in range(8):
        acc = None
        for j in range(NH):
            r = s * NH + j
            term = p_ref[0, r * 24:r * 24 + NH, :] * u_ref[kme, half, 0, 0, r:r + 1, :]
            acc = term if acc is None else acc + term
        g_ref[s * NH:s * NH + NH, :] = acc
    for i in range(5):
        v = [g_ref[8 * t:8 * t + 8, :] for t in ((4 * i, 4 * i + 1, 4 * i + 2, 4 * i + 3) if i < 4 else (16, 17, 16, 17))]
        for d, u in enumerate(fold4(v)):
            pk[d, 8 * i:8 * i + 8, :] = u

    def kcopy(rel):
        dev = (partner, pairdev, diagdev)[rel]
        d = (par * 2 + 1 - core, (1 - par) * 2 + 1 - core, (1 - par) * 2 + core)[rel]
        return remote(pk.at[d], rk.at[rel], ks_s, ks_r.at[rel], dev)

    for rel in (2, 1, 0):
        kcopy(rel).start()

    def unpack(ref, q):
        for t in range(18):
            tile = ref[8 * (t // 4):8 * (t // 4) + 8, :]
            if t % 4:
                tile = pltpu.roll(tile, 128 - 32 * (t % 4), 1)
            t_ref[pl.ds(pl.multiple_of(q * 144 + t * 8, 8), 8), :] = tile

    unpack(pk.at[par * 2 + core], quarter)
    for rel, q in ((0, par * 2 + 1 - half), (1, (1 - par) * 2 + half), (2, 3 - quarter)):
        kcopy(rel).wait_recv()
        unpack(rk.at[rel], q)
    o_ref[...] = jnp.transpose(t_ref[...])[:32, :]
    for whole, sem in ((d_ref, ds_s), (ra1, a1s), (rb1, b1s), (rc1, c1s), (ra2, a2s), (rb2, b2s), (rc2, c2s),
                       (ra3, a3s), (rb3, b3s), (rc3, c3s), (rk, ks_s)):
        remote(whole, whole, sem, ks_r.at[0], partner).wait_send()


def shards(projectors, wavefunctions, coupling, atom_order):
    a = projectors.reshape(KLOC, NKB)
    w = wavefunctions.reshape(KLOC, BANDS)
    f32 = jnp.float32
    dma = pltpu.SemaphoreType.DMA
    any_spec = pl.BlockSpec(memory_space=pltpu.HBM)
    sems = []
    for shape in ((2, 8), (2, 8), (6, 4), (2, 4), (2, 4), (2, 2), (3,), (3,), (2,), (3,)):
        sems += [dma, dma(shape)]
    out = pl.pallas_call(
        kernel,
        out_shape=pltpu.VMEM((32, 576), f32),
        in_specs=[any_spec, any_spec, any_spec, any_spec],
        out_specs=pl.BlockSpec(memory_space=pltpu.VMEM),
        scratch_shapes=[
            pltpu.VMEM((2, NKB + 8, 128), f32),
            pltpu.VMEM((8, 2, 4, 4, 144, 128), f32),
            pltpu.VMEM((8, 4, 4, 144, 128), f32),
            pltpu.VMEM((KLOC, NKB), jnp.bfloat16),
            pltpu.VMEM((4, KLOC, 128), jnp.bfloat16),
            pltpu.VMEM((NH, NH, 32), f32),
            pltpu.VMEM((144, 128), f32),
            pltpu.VMEM((4, 40, 128), f32),
            pltpu.VMEM((3, 40, 128), f32),
            pltpu.VMEM((576, 128), f32),
            pltpu.VMEM((3, 8, 4, 48, 128), f32),
            pltpu.VMEM((3, 8, 4, 48, 128), f32),
            pltpu.VMEM((7, 4, 4, 48, 128), f32),
            pltpu.VMEM((3, 8, 48, 128), f32),
            pltpu.VMEM((3, 8, 48, 128), f32),
            pltpu.VMEM((3, 4, 48, 128), f32),
            pltpu.VMEM((7, 48, 128), f32),
            pltpu.VMEM((7, 48, 128), f32),
            pltpu.VMEM((3, 48, 128), f32),
            pltpu.SMEM((512,), jnp.int32),
            dma((5,)),
            dma((4,)),
            dma,
            dma,
            dma,
            dma((5, 3)),
        ] + sems,
        compiler_params=pltpu.CompilerParams(
            vmem_limit_bytes=62500000, collective_id=0, has_side_effects=True),
        cost_estimate=pl.CostEstimate(flops=2 * KLOC * NKB * BANDS, bytes_accessed=10 * 2**20, transcendentals=0),
    )(atom_order, a, w, coupling.transpose(1, 2, 0))
    return out.T


def solution(mesh):
    return jax.shard_map(
        shards,
        mesh=mesh,
        in_specs=(
            P(None, ("gr", "gc"), None),
            P(None, ("gr", "gc"), None),
            P("gc", None, None),
            P(),
        ),
        out_specs=P("gc", "gr"),
        check_vma=False,
    )
```

```python
import functools

import jax
import jax.numpy as jnp
from jax import lax
from jax.experimental import pallas as pl
from jax.experimental.pallas import tpu as pltpu
from jax.sharding import PartitionSpec as P

MESH = pl.DeviceIdType.MESH
NH = 18
BANDS = 512
NKB = 9216
KLOC = 512
MC = 1536
CHUNKS = NKB // MC
ROWS = (slice(0, 48), slice(48, 96), slice(96, 144))


def fold4(v):
    lane = lax.broadcasted_iota(jnp.int32, v[0].shape, 1)
    low = lane < 64
    even = (lane // 32) % 2 == 0
    roll = pltpu.roll
    lo = [jnp.where(low, v[q], roll(v[q + 2], 64, 1)) for q in range(2)]
    hi = [jnp.where(low, roll(v[q], 64, 1), v[q + 2]) for q in range(2)]
    u = []
    for a, b in (lo, hi):
        u.append(jnp.where(even, a, roll(b, 32, 1)))
        u.append(jnp.where(even, roll(a, 96, 1), b))
    return u


def kernel(order_hbm, a_hbm, w_hbm, c_hbm, o_ref,
           p_ref, u_ref, d_ref, a_v, w_v, c_v, g_ref, pk, rk, t_ref,
           ra1, rb1, rc1, ra2, rb2, rc2, ra3, rb3, rc3,
           order, asem, wsem, csem, osem, ds_s, ds_r,
           a1s, a1r, b1s, b1r, c1s, c1r, a2s, a2r, b2s, b2r, c2s, c2r,
           a3s, a3r, b3s, b3r, c3s, c3r, ks_s, ks_r):
    gr, gc = lax.axis_index("gr"), lax.axis_index("gc")
    z, core = gr // 2, gr % 2
    x, y = gc // 4, gc % 4
    half = (core + x + y + z) % 2
    sg = 1 - 2 * half
    par = z % 2
    zt = z // 2
    quarter = par * 2 + half

    def xdev(d):
        return (z * 2 + (core + d + 4) % 2, ((x + d + 4) % 4) * 4 + y)

    def ydev(d):
        return (z * 2 + (core + d + 4) % 2, x * 4 + (y + d + 4) % 4)

    def pdev(d):
        return (z * 2 + (core + d + 4) % 2, (1 - half) * xdev(d)[1] + half * ydev(d)[1])

    def qdev(d):
        return (z * 2 + (core + d + 4) % 2, half * xdev(d)[1] + (1 - half) * ydev(d)[1])

    def zdev(d):
        return (((z + d + 8) % 8) * 2 + (core + d + 8) % 2, gc)

    partner = (z * 2 + 1 - core, gc)
    zpair = z + 1 - 2 * par
    pairdev = (zpair * 2 + 1 - core, gc)
    diagdev = (zpair * 2 + core, gc)

    tiles = [(zt + 2) % 4, (zt + 1 + 2 * par) % 4, (zt + 3 - 2 * par) % 4, zt]

    def kof(d):
        rel = ((par + d + 8) // 2) % 4
        odd = rel % 2
        up = rel // 2
        pos = odd * (1 + (par + up) % 2) + (1 - odd) * (3 - 3 * up)
        return 2 * pos + (par + d + 8 + par * (1 - odd) * up) % 2

    kme = 6 + par

    def acopy(m):
        cols = pl.ds(pl.multiple_of(m * MC, 128), MC)
        return pltpu.make_async_copy(a_hbm.at[:, cols], a_v.at[:, cols], asem.at[m % 5])

    def wcopy(t):
        cols = pl.ds(pl.multiple_of(tiles[t] * 128, 128), 128)
        return pltpu.make_async_copy(w_hbm.at[:, cols], w_v.at[t], wsem.at[t])

    for t in range(2):
        wcopy(t).start()
    acopy(0).start()
    ocopy = pltpu.make_async_copy(order_hbm, order, osem)
    ccopy = pltpu.make_async_copy(c_hbm, c_v, csem)
    barrier = pltpu.get_barrier_semaphore()
    greet = [xdev(1), xdev(-1), xdev(2), ydev(1), ydev(-1), ydev(2), zdev(1), zdev(-1), zdev(2), zdev(-2), partner, diagdev]
    for dev in greet:
        pl.semaphore_signal(barrier, inc=1, device_id=dev, device_id_type=MESH)
    acopy(1).start()
    for t in range(2):
        wcopy(t).wait()
    for m in range(2, 4):
        acopy(m).start()
    for t in range(2, 4):
        wcopy(t).start()
    ocopy.start()

    def matmul(h, first, last, wait):
        w = jnp.concatenate([w_v[2 * h], w_v[2 * h + 1]], axis=1)

        @pl.loop(first, last)
        def _(m):
            if wait:
                acopy(m).wait()

                @pl.when(m + 4 < CHUNKS)
                def _():
                    acopy(m + 4).start()
            lhs = a_v[:, pl.ds(pl.multiple_of(m * MC, 128), MC)]
            r = lax.dot_general(lhs, w, (((0,), (0,)), ((), ())), preferred_element_type=jnp.float32)
            rows = pl.ds(pl.multiple_of(m * MC, 128), MC)
            p_ref[0, rows, :] = r[:, :128]
            p_ref[1, rows, :] = r[:, 128:]

    def gather(kk, zs):
        step = 1

        @pl.loop(0, 16 // step)
        def _(i):
            for g in [i * step + j for j in range(step)]:
                for k, zl in zs:
                    for h in range(2):
                        way = 1 - 2 * h
                        rx = (way * (g // 4 - x) + 4) % 4
                        ry = (way * (g % 4 - y) + 4) % 4
                        p, q = (rx, ry) if h == 0 else (ry, rx)
                        for s in range(8):
                            start = order[g * 32 + (2 * zl + h) * 8 + s] * NH
                            n = 24 if s < 7 else 18
                            u_ref[2 * kk + k, h, p, q, s * 18:s * 18 + n, :] = p_ref[kk % 2, pl.ds(start, n), :]

    def remote(src, dst, ssem, rsem, dev):
        return pltpu.make_async_remote_copy(src_ref=src, dst_ref=dst, send_sem=ssem, recv_sem=rsem,
                                            device_id=dev, device_id_type=MESH)

    def dcopy(kk, c):
        ks = pl.ds(2 * kk, 2)
        return remote(u_ref.at[ks, 1 - half, :, :, ROWS[c], :], d_ref.at[ks, :, :, ROWS[c], :],
                      ds_s, ds_r.at[kk, c], partner)

    def dfirst(h, c):
        return remote(u_ref.at[h, 1 - half, :, :, ROWS[c], :], d_ref.at[h, :, :, ROWS[c], :],
                      ds_s, ds_r.at[4 * h, c], partner)

    def make(kk):
        gather(kk, ((0, 0), (1, 1)))
        if kk == 3:
            ccopy.wait()
        for c in (0, 1, 2):
            dcopy(kk, c).start()

    def make_first(h):
        gather(0, ((h, (par + h) % 2),))
        for c in (0, 1, 2):
            dfirst(h, c).start()

    def ring4(own, add, slot, ssem, rsem, dev, direct=False):
        def copy(j):
            if direct:
                return remote(own((2, 1, 3)[j]), slot(j), ssem, rsem(0), dev((2, sg, -sg)[j]))
            return remote(own((2, 1, 3)[j]), slot(j), ssem, rsem(min(j, 1)), dev(-sg if j == 2 else sg))

        def far():
            add(2, [])
            copy(0).start()

        def back():
            add(3, [])
            copy(2).start()

        def second():
            if not direct:
                copy(0).wait_recv()
                add(1, [slot(0)])
            copy(1).start()

        def end():
            first = 0 if direct else 1
            landed = slot(pl.ds(first, 3 - first))
            remote(landed, landed, ssem, rsem(first), dev(sg)).wait_recv()
            add(0, [slot(j) for j in range(first, 3)])

        return far, back, second, end

    def ring8(own, add, slot, ssem, rsem):
        far = {0: 4 * sg, 1: 3 * sg, 2: 2 * sg, 3: sg, 5: -3 * sg, 6: -2 * sg, 4: -sg}
        sem = {0: 0, 1: 1, 2: 2, 3: 3, 4: 3, 5: 4, 6: 5}

        def copy(j):
            return remote(own(far[j]), slot(j), ssem, rsem(sem[j]), zdev(sg if j < 4 else -sg))

        def start(j):
            def run():
                add(far[j], [])
                copy(j).start()
            return run

        def step(before, j):
            def run():
                copy(before).wait_recv()
                add(far[j], [slot(before)])
                copy(j).start()
            return run

        def end():
            remote(slot(pl.ds(3, 2)), slot(pl.ds(3, 2)), ssem, rsem(3), zdev(sg)).wait_recv()
            add(0 * sg, [slot(3), slot(4)])

        return start(0), start(5), step(0, 1), step(1, 2), step(2, 3), step(5, 6), step(6, 4), end

    def ring8_short(own, add, slot, ssem, rsem):
        far = (4 * sg, 3 * sg, -3 * sg, -2 * sg, 2 * sg, sg, -sg)
        dev = (2 * sg, sg, -2 * sg, -sg, 2 * sg, sg, -sg)
        group = (0, 0, 1, 1, 2, 2, 2)

        def copy(j):
            return remote(own(far[j]), slot(j), ssem, rsem(group[j]), zdev(dev[j]))

        def wait(first, n):
            landed = slot(pl.ds(first, n))
            remote(landed, landed, ssem, rsem(group[first]), zdev(sg)).wait_recv()
            return [slot(j) for j in range(first, first + n)]

        def join(first, j):
            def run():
                add(far[j], wait(first, 2))
                copy(j).start()
            return run

        def end():
            add(0 * sg, wait(4, 3))

        return (copy(0).start, copy(1).start, copy(2).start, copy(3).start, join(0, 4), copy(5).start, join(2, 6), end)

    def adder(own, more=None):
        def add(dest, extra):
            refs = ([more(dest)] if more is not None else []) + extra
            if refs:
                ref = own(dest)
                total = ref[...]
                for other in refs:
                    total = total + other[...]
                ref[...] = total
        return add

    def a1(k):
        own = lambda r: u_ref.at[k, half, r, :, ROWS[0], :]
        more = lambda r: d_ref.at[k, r, :, ROWS[0], :]
        return ring4(own, adder(own, more), lambda j: ra1.at[j, k],
                     a1s, lambda j: a1r.at[j, k], pdev)

    def b1(k):
        own = lambda r: u_ref.at[k, half, :, r, ROWS[1], :]
        more = lambda r: d_ref.at[k, :, r, ROWS[1], :]
        return ring4(own, adder(own, more), lambda j: rb1.at[j, k],
                     b1s, lambda j: b1r.at[j, k], qdev)

    def c1(i):
        r = (2, 3, 1, 0)[i]
        own = lambda d: u_ref.at[kof(d), half, r, :, ROWS[2], :]
        more = lambda d: d_ref.at[kof(d), r, :, ROWS[2], :]
        return ring8(own, adder(own, more), lambda j: rc1.at[j, r],
                     c1s, lambda j: c1r.at[j, r])

    def a2(i):
        ks = pl.ds(2 * i, 2)
        own = lambda r: u_ref.at[ks, half, 0, r, ROWS[0], :]
        return ring4(own, adder(own), lambda j: ra2.at[j, ks],
                     a2s, lambda j: a2r.at[j, i], qdev, direct=i in (3,))

    def b2(i):
        ks = pl.ds(2 * i, 2)
        own = lambda r: u_ref.at[ks, half, r, 0, ROWS[1], :]
        return ring4(own, adder(own), lambda j: rb2.at[j, ks],
                     b2s, lambda j: b2r.at[j, i], pdev, direct=i in (3,))

    def c2(i):
        ys = pl.ds(2 - 2 * i, 2)
        own = lambda r: u_ref.at[kme, half, r, ys, ROWS[2], :]
        return ring4(own, adder(own), lambda j: rc2.at[j, ys],
                     c2s, lambda j: c2r.at[j, i], pdev)

    def c3():
        own = lambda r: u_ref.at[kme, half, 0, r, ROWS[2], :]
        return ring4(own, adder(own), lambda j: rc3.at[j],
                     c3s, lambda j: c3r.at[j], qdev, direct=True)

    def a3():
        own = lambda d: u_ref.at[kof(d), half, 0, 0, ROWS[0], :]
        return ring8_short(own, adder(own), lambda j: ra3.at[j], a3s, lambda j: a3r.at[j])

    def b3():
        own = lambda d: u_ref.at[kof(d), half, 0, 0, ROWS[1], :]
        return ring8_short(own, adder(own), lambda j: rb3.at[j], b3s, lambda j: b3r.at[j])

    def spread(i):
        for j in range(3 * i, 3 * i + 3):
            v = 2.0 * c_v[:, j, :]
            v = pltpu.roll(jnp.concatenate([v, v, v, v], axis=1), 128 - 8 * quarter, 1)
            for s in range(8):
                r = (s * NH + j) * 24
                p_ref[0, r:r + NH, :] = jnp.broadcast_to(v[:, s:s + 1], (NH, 128))

    def bar():
        ocopy.wait()
        ccopy.start()
        for t in range(2, 4):
            wcopy(t).wait()
        pl.semaphore_wait(barrier, len(greet))

    def each(f, n):
        return [functools.partial(f, i) for i in range(n)]

    m0 = functools.partial(matmul, 0, 0, CHUNKS, True)
    m1 = [functools.partial(matmul, 1, 2 * i, 2 * i + 2, False) for i in range(3)]
    g0, g, cb = each(make_first, 2), each(make, 4), each(spread, 6)
    w0 = [[functools.partial(lambda h, c: dfirst(h, c).wait_recv(), h, c) for c in range(3)] for h in range(2)]
    wd = [[functools.partial(lambda k, c: dcopy(k, c).wait_recv(), k, c) for c in range(3)] for k in range(4)]
    ra, rb, rc = [a1(k) for k in range(8)], [b1(k) for k in range(8)], [c1(i) for i in range(4)]
    sa, sb, sc = [a2(i) for i in range(4)], [b2(i) for i in range(4)], [c2(i) for i in range(2)]
    ta, tb, tc = a3(), b3(), c3()
    for run in (
        m0, bar, g0[0], g0[1], w0[0][0], ra[0][0], ra[0][1], g[1], w0[0][2], w0[0][1], rc[0][0], rb[0][1], rc[3][0],
        rb[0][0], rc[2][0], w0[1][0], ra[1][0], ra[1][1], m1[0], w0[1][1], rb[1][0], rb[1][1], m1[1], ra[0][2],
        wd[1][0], ra[3][1], w0[1][2], rc[1][0], ra[3][0], ra[2][1], m1[2], wd[1][1], rb[2][0], rb[3][0], ra[2][0],
        wd[1][2], rc[0][2], g[2], rc[0][1], rb[0][2], ra[1][2], rb[2][1], rb[1][2], rc[3][1], rb[3][1], rc[1][2],
        g[3], rc[2][1], rc[1][1], wd[2][0], cb[4], cb[2], ra[5][1], wd[2][1], rb[4][0], ra[4][0], ra[2][2], ra[0][3],
        wd[2][2], rb[5][0], rb[3][2], rc[3][2], cb[1], ra[5][0], ra[1][3], rc[0][5], wd[3][0], rb[0][3], wd[3][1],
        ra[3][2], rc[2][2], rc[0][3], rb[7][0], rb[1][3], sb[0][0], cb[0], wd[3][2], rc[1][3], ra[7][0], rb[5][1],
        rb[4][1], rb[4][2], rc[1][5], rb[2][2], rb[5][2], ra[5][2], ra[3][3], rc[2][3], rc[2][5], ra[4][1], rc[3][3],
        ra[4][2], sa[0][0], ra[7][1], ra[2][3], ra[6][0], rc[1][6], rc[0][4], rb[3][3], sb[0][2], rb[2][3], sa[1][0],
        sa[0][1], ra[7][2], sb[0][1], sb[1][0], ra[6][1], rc[0][6], rb[6][0], ra[5][3], ra[4][3], sa[1][1], rb[6][1],
        rb[5][3], rb[4][3], cb[5], sb[2][0], sa[2][0], rb[7][1], sa[0][2], rc[1][4], rb[7][2], sa[1][2], rc[3][5],
        ra[6][2], rc[2][6], rb[6][2], rc[2][4], sa[2][2], rc[0][7], rc[3][4], sc[0][0], sb[1][2], sb[1][1], ra[7][3],
        sb[2][1], sb[2][2], sc[1][0], sa[0][3], sb[0][3], ta[0], tb[0], rc[1][7], sa[2][1], sa[1][3], cb[3], sc[0][1],
        ta[1], rc[3][6], ra[6][3], sa[3][0], sa[3][1], sa[3][2], rb[7][3], rb[6][3], sb[3][0], ta[2], sb[1][3],
        sc[1][1], sb[3][1], rc[2][7], tb[2], sc[0][2], tb[1], sb[3][2], sa[2][3], ta[3], sb[2][3], tb[3], sc[1][2],
        ta[4], rc[3][7], tb[4], sc[0][3], tc[1], tc[0], sa[3][3], ta[5], sb[3][3], tb[5], ta[6], sc[1][3], tc[2],
        tb[6], ta[7], tc[3], tb[7],
    ):
        run()

    for s in range(8):
        acc = None
        for j in range(NH):
            r = s * NH + j
            term = p_ref[0, r * 24:r * 24 + NH, :] * u_ref[kme, half, 0, 0, r:r + 1, :]
            acc = term if acc is None else acc + term
        g_ref[s * NH:s * NH + NH, :] = acc
    for i in range(5):
        v = [g_ref[8 * t:8 * t + 8, :] for t in ((4 * i, 4 * i + 1, 4 * i + 2, 4 * i + 3) if i < 4 else (16, 17, 16, 17))]
        for d, u in enumerate(fold4(v)):
            pk[d, 8 * i:8 * i + 8, :] = u

    def kcopy(rel):
        dev = (partner, pairdev, diagdev)[rel]
        d = (par * 2 + 1 - core, (1 - par) * 2 + 1 - core, (1 - par) * 2 + core)[rel]
        return remote(pk.at[d], rk.at[rel], ks_s, ks_r.at[rel], dev)

    for rel in (2, 1, 0):
        kcopy(rel).start()

    def unpack(ref, q):
        for t in range(18):
            tile = ref[8 * (t // 4):8 * (t // 4) + 8, :]
            if t % 4:
                tile = pltpu.roll(tile, 128 - 32 * (t % 4), 1)
            t_ref[pl.ds(pl.multiple_of(q * 144 + t * 8, 8), 8), :] = tile

    unpack(pk.at[par * 2 + core], quarter)
    for rel, q in ((0, par * 2 + 1 - half), (1, (1 - par) * 2 + half), (2, 3 - quarter)):
        kcopy(rel).wait_recv()
        unpack(rk.at[rel], q)
    o_ref[...] = jnp.transpose(t_ref[...])[:32, :]
    for whole, sem in ((d_ref, ds_s), (ra1, a1s), (rb1, b1s), (rc1, c1s), (ra2, a2s), (rb2, b2s), (rc2, c2s),
                       (ra3, a3s), (rb3, b3s), (rc3, c3s), (rk, ks_s)):
        remote(whole, whole, sem, ks_r.at[0], partner).wait_send()


def shards(projectors, wavefunctions, coupling, atom_order):
    a = projectors.reshape(KLOC, NKB)
    w = wavefunctions.reshape(KLOC, BANDS)
    f32 = jnp.float32
    dma = pltpu.SemaphoreType.DMA
    any_spec = pl.BlockSpec(memory_space=pltpu.HBM)
    sems = []
    for shape in ((2, 8), (2, 8), (6, 4), (2, 4), (2, 4), (2, 2), (3,), (3,), (2,), (3,)):
        sems += [dma, dma(shape)]
    out = pl.pallas_call(
        kernel,
        out_shape=pltpu.VMEM((32, 576), f32),
        in_specs=[any_spec, any_spec, any_spec, any_spec],
        out_specs=pl.BlockSpec(memory_space=pltpu.VMEM),
        scratch_shapes=[
            pltpu.VMEM((2, NKB + 8, 128), f32),
            pltpu.VMEM((8, 2, 4, 4, 144, 128), f32),
            pltpu.VMEM((8, 4, 4, 144, 128), f32),
            pltpu.VMEM((KLOC, NKB), jnp.bfloat16),
            pltpu.VMEM((4, KLOC, 128), jnp.bfloat16),
            pltpu.VMEM((NH, NH, 32), f32),
            pltpu.VMEM((144, 128), f32),
            pltpu.VMEM((4, 40, 128), f32),
            pltpu.VMEM((3, 40, 128), f32),
            pltpu.VMEM((576, 128), f32),
            pltpu.VMEM((3, 8, 4, 48, 128), f32),
            pltpu.VMEM((3, 8, 4, 48, 128), f32),
            pltpu.VMEM((7, 4, 4, 48, 128), f32),
            pltpu.VMEM((3, 8, 48, 128), f32),
            pltpu.VMEM((3, 8, 48, 128), f32),
            pltpu.VMEM((3, 4, 48, 128), f32),
            pltpu.VMEM((7, 48, 128), f32),
            pltpu.VMEM((7, 48, 128), f32),
            pltpu.VMEM((3, 48, 128), f32),
            pltpu.SMEM((512,), jnp.int32),
            dma((5,)),
            dma((4,)),
            dma,
            dma,
            dma,
            dma((5, 3)),
        ] + sems,
        compiler_params=pltpu.CompilerParams(
            vmem_limit_bytes=62500000, collective_id=0, has_side_effects=True),
        cost_estimate=pl.CostEstimate(flops=2 * KLOC * NKB * BANDS, bytes_accessed=10 * 2**20, transcendentals=0),
    )(atom_order, a, w, coupling.transpose(1, 2, 0))
    return out.T


def solution(mesh):
    return jax.shard_map(
        shards,
        mesh=mesh,
        in_specs=(
            P(None, ("gr", "gc"), None),
            P(None, ("gr", "gc"), None),
            P("gc", None, None),
            P(),
        ),
        out_specs=P("gc", "gr"),
        check_vma=False,
    )
```

```python
import functools

import jax
import jax.numpy as jnp
from jax import lax
from jax.experimental import pallas as pl
from jax.experimental.pallas import tpu as pltpu
from jax.sharding import PartitionSpec as P

MESH = pl.DeviceIdType.MESH
NH = 18
BANDS = 512
NKB = 9216
KLOC = 512
MC = 1536
CHUNKS = NKB // MC
ROWS = (slice(0, 48), slice(48, 96), slice(96, 144))


def fold4(v):
    lane = lax.broadcasted_iota(jnp.int32, v[0].shape, 1)
    low = lane < 64
    even = (lane // 32) % 2 == 0
    roll = pltpu.roll
    lo = [jnp.where(low, v[q], roll(v[q + 2], 64, 1)) for q in range(2)]
    hi = [jnp.where(low, roll(v[q], 64, 1), v[q + 2]) for q in range(2)]
    u = []
    for a, b in (lo, hi):
        u.append(jnp.where(even, a, roll(b, 32, 1)))
        u.append(jnp.where(even, roll(a, 96, 1), b))
    return u


def kernel(order_hbm, a_hbm, w_hbm, c_hbm, o_ref,
           p_ref, u_ref, d_ref, a_v, w_v, c_v, g_ref, pk, rk, t_ref,
           ra1, rb1, rc1, ra2, rb2, rc2, ra3, rb3, rc3,
           order, asem, wsem, csem, osem, ds_s, ds_r,
           a1s, a1r, b1s, b1r, c1s, c1r, a2s, a2r, b2s, b2r, c2s, c2r,
           a3s, a3r, b3s, b3r, c3s, c3r, ks_s, ks_r):
    gr, gc = lax.axis_index("gr"), lax.axis_index("gc")
    z, core = gr // 2, gr % 2
    x, y = gc // 4, gc % 4
    half = (core + x + y + z) % 2
    sg = 1 - 2 * half
    par = z % 2
    zt = z // 2
    quarter = par * 2 + half

    def xdev(d):
        return (z * 2 + (core + d + 4) % 2, ((x + d + 4) % 4) * 4 + y)

    def ydev(d):
        return (z * 2 + (core + d + 4) % 2, x * 4 + (y + d + 4) % 4)

    def pdev(d):
        return (z * 2 + (core + d + 4) % 2, (1 - half) * xdev(d)[1] + half * ydev(d)[1])

    def qdev(d):
        return (z * 2 + (core + d + 4) % 2, half * xdev(d)[1] + (1 - half) * ydev(d)[1])

    def zdev(d):
        return (((z + d + 8) % 8) * 2 + (core + d + 8) % 2, gc)

    partner = (z * 2 + 1 - core, gc)
    zpair = z + 1 - 2 * par
    pairdev = (zpair * 2 + 1 - core, gc)
    diagdev = (zpair * 2 + core, gc)

    tiles = [(zt + 2) % 4, (zt + 1 + 2 * par) % 4, (zt + 3 - 2 * par) % 4, zt]

    def kof(d):
        rel = ((par + d + 8) // 2) % 4
        odd = rel % 2
        up = rel // 2
        pos = odd * (1 + (par + up) % 2) + (1 - odd) * (3 - 3 * up)
        return 2 * pos + (par + d + 8 + par * (1 - odd) * up) % 2

    kme = 6 + par

    def acopy(m):
        cols = pl.ds(pl.multiple_of(m * MC, 128), MC)
        return pltpu.make_async_copy(a_hbm.at[:, cols], a_v.at[:, cols], asem.at[m % 5])

    def wcopy(t):
        cols = pl.ds(pl.multiple_of(tiles[t] * 128, 128), 128)
        return pltpu.make_async_copy(w_hbm.at[:, cols], w_v.at[t], wsem.at[t])

    for t in range(2):
        wcopy(t).start()
    acopy(0).start()
    ocopy = pltpu.make_async_copy(order_hbm, order, osem)
    ccopy = pltpu.make_async_copy(c_hbm, c_v, csem)
    barrier = pltpu.get_barrier_semaphore()
    greet = [xdev(1), xdev(-1), xdev(2), ydev(1), ydev(-1), ydev(2), zdev(1), zdev(-1), zdev(2), zdev(-2), partner, diagdev]
    for dev in greet:
        pl.semaphore_signal(barrier, inc=1, device_id=dev, device_id_type=MESH)
    acopy(1).start()
    for t in range(2):
        wcopy(t).wait()
    for m in range(2, 4):
        acopy(m).start()
    for t in range(2, 4):
        wcopy(t).start()
    ocopy.start()

    def matmul(h, first, last, wait):
        w = jnp.concatenate([w_v[2 * h], w_v[2 * h + 1]], axis=1)

        @pl.loop(first, last)
        def _(m):
            if wait:
                acopy(m).wait()

                @pl.when(m + 4 < CHUNKS)
                def _():
                    acopy(m + 4).start()
            lhs = a_v[:, pl.ds(pl.multiple_of(m * MC, 128), MC)]
            r = lax.dot_general(lhs, w, (((0,), (0,)), ((), ())), preferred_element_type=jnp.float32)
            rows = pl.ds(pl.multiple_of(m * MC, 128), MC)
            p_ref[0, rows, :] = r[:, :128]
            p_ref[1, rows, :] = r[:, 128:]

    def gather(kk, zs):
        step = 1

        @pl.loop(0, 16 // step)
        def _(i):
            for g in [i * step + j for j in range(step)]:
                for k, zl in zs:
                    for h in range(2):
                        way = 1 - 2 * h
                        rx = (way * (g // 4 - x) + 4) % 4
                        ry = (way * (g % 4 - y) + 4) % 4
                        p, q = (rx, ry) if h == 0 else (ry, rx)
                        for s in range(8):
                            start = order[g * 32 + (2 * zl + h) * 8 + s] * NH
                            n = 24 if s < 7 else 18
                            u_ref[2 * kk + k, h, p, q, s * 18:s * 18 + n, :] = p_ref[kk % 2, pl.ds(start, n), :]

    def remote(src, dst, ssem, rsem, dev):
        return pltpu.make_async_remote_copy(src_ref=src, dst_ref=dst, send_sem=ssem, recv_sem=rsem,
                                            device_id=dev, device_id_type=MESH)

    def dcopy(kk, c):
        ks = pl.ds(2 * kk, 2)
        return remote(u_ref.at[ks, 1 - half, :, :, ROWS[c], :], d_ref.at[ks, :, :, ROWS[c], :],
                      ds_s, ds_r.at[kk, c], partner)

    def dfirst(h, c):
        return remote(u_ref.at[h, 1 - half, :, :, ROWS[c], :], d_ref.at[h, :, :, ROWS[c], :],
                      ds_s, ds_r.at[4 * h, c], partner)

    def make(kk):
        gather(kk, ((0, 0), (1, 1)))
        if kk == 3:
            ccopy.wait()
        for c in (0, 1, 2):
            dcopy(kk, c).start()

    def make_first(h):
        gather(0, ((h, (par + h) % 2),))
        for c in (0, 1, 2):
            dfirst(h, c).start()

    def ring4(own, add, slot, ssem, rsem, dev, direct=False):
        def copy(j):
            if direct:
                return remote(own((2, 1, 3)[j]), slot(j), ssem, rsem(0), dev((2, sg, -sg)[j]))
            return remote(own((2, 1, 3)[j]), slot(j), ssem, rsem(min(j, 1)), dev(-sg if j == 2 else sg))

        def far():
            add(2, [])
            copy(0).start()

        def back():
            add(3, [])
            copy(2).start()

        def second():
            if not direct:
                copy(0).wait_recv()
                add(1, [slot(0)])
            copy(1).start()

        def end():
            first = 0 if direct else 1
            landed = slot(pl.ds(first, 3 - first))
            remote(landed, landed, ssem, rsem(first), dev(sg)).wait_recv()
            add(0, [slot(j) for j in range(first, 3)])

        return far, back, second, end

    def ring8(own, add, slot, ssem, rsem):
        far = {0: 4 * sg, 1: 3 * sg, 2: 2 * sg, 3: sg, 5: -3 * sg, 6: -2 * sg, 4: -sg}
        sem = {0: 0, 1: 1, 2: 2, 3: 3, 4: 3, 5: 4, 6: 5}

        def copy(j):
            return remote(own(far[j]), slot(j), ssem, rsem(sem[j]), zdev(sg if j < 4 else -sg))

        def start(j):
            def run():
                add(far[j], [])
                copy(j).start()
            return run

        def step(before, j):
            def run():
                copy(before).wait_recv()
                add(far[j], [slot(before)])
                copy(j).start()
            return run

        def end():
            remote(slot(pl.ds(3, 2)), slot(pl.ds(3, 2)), ssem, rsem(3), zdev(sg)).wait_recv()
            add(0 * sg, [slot(3), slot(4)])

        return start(0), start(5), step(0, 1), step(1, 2), step(2, 3), step(5, 6), step(6, 4), end

    def ring8_short(own, add, slot, ssem, rsem):
        far = (4 * sg, 3 * sg, -3 * sg, -2 * sg, 2 * sg, sg, -sg)
        dev = (2 * sg, sg, -2 * sg, -sg, 2 * sg, sg, -sg)
        group = (0, 0, 1, 1, 2, 2, 2)

        def copy(j):
            return remote(own(far[j]), slot(j), ssem, rsem(group[j]), zdev(dev[j]))

        def wait(first, n):
            landed = slot(pl.ds(first, n))
            remote(landed, landed, ssem, rsem(group[first]), zdev(sg)).wait_recv()
            return [slot(j) for j in range(first, first + n)]

        def join(first, j):
            def run():
                add(far[j], wait(first, 2))
                copy(j).start()
            return run

        def end():
            add(0 * sg, wait(4, 3))

        return (copy(0).start, copy(1).start, copy(2).start, copy(3).start, join(0, 4), copy(5).start, join(2, 6), end)

    def adder(own, more=None):
        def add(dest, extra):
            refs = ([more(dest)] if more is not None else []) + extra
            if refs:
                ref = own(dest)
                total = ref[...]
                for other in refs:
                    total = total + other[...]
                ref[...] = total
        return add

    def a1(k):
        own = lambda r: u_ref.at[k, half, r, :, ROWS[0], :]
        more = lambda r: d_ref.at[k, r, :, ROWS[0], :]
        return ring4(own, adder(own, more), lambda j: ra1.at[j, k],
                     a1s, lambda j: a1r.at[j, k], pdev)

    def b1(k):
        own = lambda r: u_ref.at[k, half, :, r, ROWS[1], :]
        more = lambda r: d_ref.at[k, :, r, ROWS[1], :]
        return ring4(own, adder(own, more), lambda j: rb1.at[j, k],
                     b1s, lambda j: b1r.at[j, k], qdev)

    def c1(i):
        r = (2, 3, 1, 0)[i]
        own = lambda d: u_ref.at[kof(d), half, r, :, ROWS[2], :]
        more = lambda d: d_ref.at[kof(d), r, :, ROWS[2], :]
        return ring8(own, adder(own, more), lambda j: rc1.at[j, r],
                     c1s, lambda j: c1r.at[j, r])

    def a2(i):
        ks = pl.ds(2 * i, 2)
        own = lambda r: u_ref.at[ks, half, 0, r, ROWS[0], :]
        return ring4(own, adder(own), lambda j: ra2.at[j, ks],
                     a2s, lambda j: a2r.at[j, i], qdev, direct=i in (3,))

    def b2(i):
        ks = pl.ds(2 * i, 2)
        own = lambda r: u_ref.at[ks, half, r, 0, ROWS[1], :]
        return ring4(own, adder(own), lambda j: rb2.at[j, ks],
                     b2s, lambda j: b2r.at[j, i], pdev, direct=i in (3,))

    def c2(i):
        ys = pl.ds(2 - 2 * i, 2)
        own = lambda r: u_ref.at[kme, half, r, ys, ROWS[2], :]
        return ring4(own, adder(own), lambda j: rc2.at[j, ys],
                     c2s, lambda j: c2r.at[j, i], pdev)

    def c3():
        own = lambda r: u_ref.at[kme, half, 0, r, ROWS[2], :]
        return ring4(own, adder(own), lambda j: rc3.at[j],
                     c3s, lambda j: c3r.at[j], qdev, direct=True)

    def a3():
        own = lambda d: u_ref.at[kof(d), half, 0, 0, ROWS[0], :]
        return ring8_short(own, adder(own), lambda j: ra3.at[j], a3s, lambda j: a3r.at[j])

    def b3():
        own = lambda d: u_ref.at[kof(d), half, 0, 0, ROWS[1], :]
        return ring8_short(own, adder(own), lambda j: rb3.at[j], b3s, lambda j: b3r.at[j])

    def spread(i):
        for j in range(3 * i, 3 * i + 3):
            v = 2.0 * c_v[:, j, :]
            v = pltpu.roll(jnp.concatenate([v, v, v, v], axis=1), 128 - 8 * quarter, 1)
            for s in range(8):
                r = (s * NH + j) * 24
                p_ref[0, r:r + NH, :] = jnp.broadcast_to(v[:, s:s + 1], (NH, 128))

    def bar():
        ocopy.wait()
        ccopy.start()
        for t in range(2, 4):
            wcopy(t).wait()
        pl.semaphore_wait(barrier, len(greet))

    def each(f, n):
        return [functools.partial(f, i) for i in range(n)]

    m0 = functools.partial(matmul, 0, 0, CHUNKS, True)
    m1 = [functools.partial(matmul, 1, 2 * i, 2 * i + 2, False) for i in range(3)]
    g0, g, cb = each(make_first, 2), each(make, 4), each(spread, 6)
    w0 = [[functools.partial(lambda h, c: dfirst(h, c).wait_recv(), h, c) for c in range(3)] for h in range(2)]
    wd = [[functools.partial(lambda k, c: dcopy(k, c).wait_recv(), k, c) for c in range(3)] for k in range(4)]
    ra, rb, rc = [a1(k) for k in range(8)], [b1(k) for k in range(8)], [c1(i) for i in range(4)]
    sa, sb, sc = [a2(i) for i in range(4)], [b2(i) for i in range(4)], [c2(i) for i in range(2)]
    ta, tb, tc = a3(), b3(), c3()
    for run in (
        m0, bar, g0[0], g0[1], w0[0][0], ra[0][0], ra[0][1], g[1], w0[0][2], w0[0][1], rc[0][0], rb[0][1], rc[3][0],
        rb[0][0], rc[2][0], w0[1][0], ra[1][0], ra[1][1], m1[0], w0[1][1], rb[1][0], rb[1][1], m1[1], ra[0][2],
        wd[1][0], ra[3][1], w0[1][2], rc[1][0], ra[3][0], ra[2][1], m1[2], wd[1][1], rb[2][0], rb[3][0], ra[2][0],
        wd[1][2], rc[0][2], g[2], rc[0][1], rb[0][2], ra[1][2], rb[2][1], rb[1][2], rc[3][1], rb[3][1], rc[1][2],
        g[3], rc[2][1], rc[1][1], wd[2][0], cb[4], cb[2], ra[5][1], wd[2][1], rb[4][0], ra[4][0], ra[2][2], ra[0][3],
        wd[2][2], rb[5][0], rb[3][2], rc[3][2], cb[1], ra[5][0], ra[1][3], rc[0][5], wd[3][0], rb[0][3], wd[3][1],
        ra[3][2], rc[2][2], rc[0][3], rb[7][0], rb[1][3], sb[0][0], cb[0], wd[3][2], rc[1][3], ra[7][0], rb[5][1],
        rb[4][1], rb[4][2], rc[1][5], rb[2][2], rb[5][2], ra[5][2], ra[3][3], rc[2][3], rc[2][5], ra[4][1], rc[3][3],
        ra[4][2], sa[0][0], ra[7][1], ra[2][3], ra[6][0], rc[1][6], rc[0][4], rb[3][3], sb[0][2], rb[2][3], sa[1][0],
        sa[0][1], ra[7][2], sb[0][1], sb[1][0], ra[6][1], rc[0][6], rb[6][0], ra[5][3], ra[4][3], sa[1][1], rb[6][1],
        rb[5][3], rb[4][3], cb[5], sb[2][0], sa[2][0], rb[7][1], sa[0][2], rc[1][4], rb[7][2], sa[1][2], rc[3][5],
        ra[6][2], rc[2][6], rb[6][2], rc[2][4], sa[2][2], rc[0][7], rc[3][4], sc[0][0], sb[1][2], sb[1][1], ra[7][3],
        sb[2][1], sb[2][2], sc[1][0], sa[0][3], sb[0][3], ta[0], tb[0], rc[1][7], sa[2][1], sa[1][3], cb[3], sc[0][1],
        ta[1], rc[3][6], ra[6][3], sa[3][0], sa[3][1], sa[3][2], rb[7][3], rb[6][3], sb[3][0], ta[2], sb[1][3],
        sc[1][1], sb[3][1], rc[2][7], tb[2], sc[0][2], tb[1], sb[3][2], sa[2][3], ta[3], sb[2][3], tb[3], sc[1][2],
        ta[4], rc[3][7], tb[4], sc[0][3], tc[1], tc[0], sa[3][3], ta[5], sb[3][3], tb[5], ta[6], sc[1][3], tc[2],
        tb[6], ta[7], tc[3],
    ):
        run()

    def couple(slots, groups):
        for s in slots:
            acc = None
            for j in range(NH):
                r = s * NH + j
                term = p_ref[0, r * 24:r * 24 + NH, :] * u_ref[kme, half, 0, 0, r:r + 1, :]
                acc = term if acc is None else acc + term
            g_ref[s * NH:s * NH + NH, :] = acc
        for i in groups:
            v = [g_ref[8 * t:8 * t + 8, :] for t in ((4 * i, 4 * i + 1, 4 * i + 2, 4 * i + 3) if i < 4 else (16, 17, 16, 17))]
            for d, u in enumerate(fold4(v)):
                pk[d, 8 * i:8 * i + 8, :] = u

    couple((0, 1, 6, 7), (0, 4))
    tb[7]()
    couple((2, 3, 4, 5), (1, 2, 3))

    def kcopy(rel):
        dev = (partner, pairdev, diagdev)[rel]
        d = (par * 2 + 1 - core, (1 - par) * 2 + 1 - core, (1 - par) * 2 + core)[rel]
        return remote(pk.at[d], rk.at[rel], ks_s, ks_r.at[rel], dev)

    for rel in (2, 1, 0):
        kcopy(rel).start()

    def unpack(ref, q):
        for t in range(18):
            tile = ref[8 * (t // 4):8 * (t // 4) + 8, :]
            if t % 4:
                tile = pltpu.roll(tile, 128 - 32 * (t % 4), 1)
            t_ref[pl.ds(pl.multiple_of(q * 144 + t * 8, 8), 8), :] = tile

    unpack(pk.at[par * 2 + core], quarter)
    for rel, q in ((0, par * 2 + 1 - half), (1, (1 - par) * 2 + half), (2, 3 - quarter)):
        kcopy(rel).wait_recv()
        unpack(rk.at[rel], q)
    o_ref[...] = jnp.transpose(t_ref[...])[:32, :]
    for whole, sem in ((d_ref, ds_s), (ra1, a1s), (rb1, b1s), (rc1, c1s), (ra2, a2s), (rb2, b2s), (rc2, c2s),
                       (ra3, a3s), (rb3, b3s), (rc3, c3s), (rk, ks_s)):
        remote(whole, whole, sem, ks_r.at[0], partner).wait_send()


def shards(projectors, wavefunctions, coupling, atom_order):
    a = projectors.reshape(KLOC, NKB)
    w = wavefunctions.reshape(KLOC, BANDS)
    f32 = jnp.float32
    dma = pltpu.SemaphoreType.DMA
    any_spec = pl.BlockSpec(memory_space=pltpu.HBM)
    sems = []
    for shape in ((2, 8), (2, 8), (6, 4), (2, 4), (2, 4), (2, 2), (3,), (3,), (2,), (3,)):
        sems += [dma, dma(shape)]
    out = pl.pallas_call(
        kernel,
        out_shape=pltpu.VMEM((32, 576), f32),
        in_specs=[any_spec, any_spec, any_spec, any_spec],
        out_specs=pl.BlockSpec(memory_space=pltpu.VMEM),
        scratch_shapes=[
            pltpu.VMEM((2, NKB + 8, 128), f32),
            pltpu.VMEM((8, 2, 4, 4, 144, 128), f32),
            pltpu.VMEM((8, 4, 4, 144, 128), f32),
            pltpu.VMEM((KLOC, NKB), jnp.bfloat16),
            pltpu.VMEM((4, KLOC, 128), jnp.bfloat16),
            pltpu.VMEM((NH, NH, 32), f32),
            pltpu.VMEM((144, 128), f32),
            pltpu.VMEM((4, 40, 128), f32),
            pltpu.VMEM((3, 40, 128), f32),
            pltpu.VMEM((576, 128), f32),
            pltpu.VMEM((3, 8, 4, 48, 128), f32),
            pltpu.VMEM((3, 8, 4, 48, 128), f32),
            pltpu.VMEM((7, 4, 4, 48, 128), f32),
            pltpu.VMEM((3, 8, 48, 128), f32),
            pltpu.VMEM((3, 8, 48, 128), f32),
            pltpu.VMEM((3, 4, 48, 128), f32),
            pltpu.VMEM((7, 48, 128), f32),
            pltpu.VMEM((7, 48, 128), f32),
            pltpu.VMEM((3, 48, 128), f32),
            pltpu.SMEM((512,), jnp.int32),
            dma((5,)),
            dma((4,)),
            dma,
            dma,
            dma,
            dma((5, 3)),
        ] + sems,
        compiler_params=pltpu.CompilerParams(
            vmem_limit_bytes=62500000, collective_id=0, has_side_effects=True),
        cost_estimate=pl.CostEstimate(flops=2 * KLOC * NKB * BANDS, bytes_accessed=10 * 2**20, transcendentals=0),
    )(atom_order, a, w, coupling.transpose(1, 2, 0))
    return out.T


def solution(mesh):
    return jax.shard_map(
        shards,
        mesh=mesh,
        in_specs=(
            P(None, ("gr", "gc"), None),
            P(None, ("gr", "gc"), None),
            P("gc", None, None),
            P(),
        ),
        out_specs=P("gc", "gr"),
        check_vma=False,
    )
```
